32 devices in a mesh: dp: 4 (over y, z), ep: 8 (over x, core).
Axes of the slice: x: 4, y: 2, z: 2, core: 2. Of those that a mesh axis runs over, the one named last changes fastest.
The devices are a block of a 4x4x8 slice.
Arguments:
- tok_x: bfloat16 [8192, 1536], P(('dp', 'ep')), parts along dimension 0
- expert_ids: int32 [8192, 8], P(('dp', 'ep')), parts along dimension 0
- gates: float32 [8192, 8], P(('dp', 'ep')), parts along dimension 0
- hot_tok: int32 [2048], P(('dp', 'ep')), parts along dimension 0
- hot_gates: float32 [2048], P(('dp', 'ep')), parts along dimension 0
- w_gate: bfloat16 [40, 1536, 512], P('ep')
- w_up: bfloat16 [40, 1536, 512], P('ep')
- w_down: bfloat16 [40, 512, 1536], P('ep')
Outputs:
- output: bfloat16 [8192, 1536], P(('dp', 'ep')), parts along dimension 0
There are 4 independent parts. The reference program is written for one: setup_inputs(seed, part) draws one part's arguments, and reference() takes and returns one part's arrays. A program takes and returns all parts, laid end to end along the dimension named above; an argument that names none is the same for every part.
All inputs are finite; a program needn't handle non-finite values.
Results may differ from the reference program's by a relative error of at most 0.00782016.
Values are sent between devices in bfloat16 or wider.
A program may use at most 768 MiB of HBM per device.

```python
import jax
import jax.numpy as jnp
from jax import lax

GROUP_SIZE = 8
TOKENS = 256
D_MODEL = 1536
D_FF = 512
EXPERTS = 40
TOP_K = 8
HOT_ROWS = 64

COLD_CAP = (TOKENS * TOP_K + EXPERTS - 2) // (EXPERTS - 1)


def draw_routing(key):
    key_rows, key_label, key_hot = jax.random.split(key, 3)
    row_perm = jax.random.permutation(key_rows, TOKENS)
    label_perm = jax.random.permutation(key_label, EXPERTS - 1)
    route_num = (row_perm[:, None] * TOP_K + jnp.arange(TOP_K)[None, :]) % (EXPERTS - 1)
    chip_ids = 1 + label_perm[route_num]
    hot_list = jax.random.permutation(key_hot, TOKENS)[:HOT_ROWS]
    return chip_ids.astype(jnp.int32), hot_list.astype(jnp.int32)


def setup_inputs(seed: int = 0, part: int = 0) -> dict:
    base_key = jax.random.key(seed)
    key_wg, key_wu, key_wd = jax.random.split(base_key, 3)
    part_key = jax.random.fold_in(base_key, part)
    key_x, key_route, key_gate, key_hot = jax.random.split(part_key, 4)
    row_count = GROUP_SIZE * TOKENS
    tok_x = jax.random.normal(key_x, (row_count, D_MODEL), jnp.float32).astype(jnp.bfloat16)
    chip_ids, hot_list = jax.vmap(draw_routing)(jax.random.split(key_route, GROUP_SIZE))
    gates = jax.random.uniform(key_gate, (row_count, TOP_K), jnp.float32, 0.5, 1.5) * TOP_K ** -0.5
    hot_gates = jax.random.uniform(key_hot, (GROUP_SIZE * HOT_ROWS,), jnp.float32, 0.5, 1.5)
    w_gate = (jax.random.normal(key_wg, (EXPERTS, D_MODEL, D_FF), jnp.float32) * D_MODEL ** -0.5).astype(jnp.bfloat16)
    w_up = (jax.random.normal(key_wu, (EXPERTS, D_MODEL, D_FF), jnp.float32) * D_MODEL ** -0.5).astype(jnp.bfloat16)
    w_down = (jax.random.normal(key_wd, (EXPERTS, D_FF, D_MODEL), jnp.float32) * D_FF ** -0.5).astype(jnp.bfloat16)
    return {'tok_x': tok_x, 'expert_ids': chip_ids.reshape(row_count, TOP_K), 'gates': gates,
            'hot_tok': hot_list.reshape(GROUP_SIZE * HOT_ROWS), 'hot_gates': hot_gates,
            'w_gate': w_gate, 'w_up': w_up, 'w_down': w_down}


def swiglu_rows(in_rows, w_gate_e, w_up_e, w_down_e):
    gate_act = jnp.dot(in_rows, w_gate_e, preferred_element_type=jnp.float32)
    up_act = jnp.dot(in_rows, w_up_e, preferred_element_type=jnp.float32)
    hidden = (jax.nn.silu(gate_act) * up_act).astype(jnp.bfloat16)
    return jnp.dot(hidden, w_down_e, preferred_element_type=jnp.float32).astype(jnp.bfloat16)


def reference(tok_x, expert_ids, gates, hot_tok, hot_gates, w_gate, w_up, w_down):
    routes = GROUP_SIZE * TOKENS * TOP_K
    flat_ids = expert_ids.reshape(routes)
    flat_gates = gates.reshape(routes)
    max_rows = GROUP_SIZE * COLD_CAP

    def expert_step(y_sum, expert_args):
        expert, w_gate_e, w_up_e, w_down_e = expert_args
        found_pos = jnp.nonzero(flat_ids == expert, size=max_rows, fill_value=routes)[0]
        in_range = found_pos < routes
        safe_pos = jnp.minimum(found_pos, routes - 1)
        tok_rows = safe_pos // TOP_K
        weight = jnp.where(in_range, flat_gates[safe_pos], 0.0)
        expert_out = swiglu_rows(tok_x[tok_rows], w_gate_e, w_up_e, w_down_e)
        y_sum = y_sum.at[tok_rows].add(weight[:, None] * expert_out.astype(jnp.float32))
        return y_sum, None

    y_start = jnp.zeros((GROUP_SIZE * TOKENS, D_MODEL), jnp.float32)
    y_sum, unused = lax.scan(expert_step, y_start, (jnp.arange(EXPERTS, dtype=jnp.int32), w_gate, w_up, w_down))
    chip_base = (jnp.arange(GROUP_SIZE * HOT_ROWS, dtype=jnp.int32) // HOT_ROWS) * TOKENS
    hot_rows_idx = chip_base + hot_tok
    hot_out = swiglu_rows(tok_x[hot_rows_idx], w_gate[0], w_up[0], w_down[0])
    y_sum = y_sum.at[hot_rows_idx].add(hot_gates[:, None] * hot_out.astype(jnp.float32))
    return y_sum.astype(jnp.bfloat16)
```

```python
import jax
import jax.numpy as jnp
from jax import lax
from jax.sharding import PartitionSpec as P


def gate_table(ids_loc, gates_loc, hot_loc, hot_g_loc, num_experts):
    num_tokens = ids_loc.shape[0]
    expert = jnp.arange(num_experts, dtype=jnp.int32)
    cold = jnp.sum(jnp.where(ids_loc[:, :, None] == expert, gates_loc[:, :, None], 0.0), axis=1)
    token = jnp.arange(num_tokens, dtype=jnp.int32)
    hot = jnp.sum(jnp.where(hot_loc[None, :] == token[:, None], hot_g_loc[None, :], 0.0), axis=1)
    return jnp.where(expert[None, :] == 0, hot[:, None], cold)


def solution(mesh):
    group_size = mesh.shape['ep']
    row_spec = P(('dp', 'ep'), None)
    list_spec = P(('dp', 'ep'))
    expert_spec = P('ep', None, None)

    def local_layer(x_loc, ids_loc, gates_loc, hot_loc, hot_g_loc, wg_loc, wu_loc, wd_loc):
        local_experts = wg_loc.shape[0]
        num_experts = local_experts * group_size
        table = gate_table(ids_loc, gates_loc, hot_loc, hot_g_loc, num_experts)
        x_all = lax.all_gather(x_loc, 'ep', axis=0, tiled=True)
        table = table.reshape(-1, group_size, local_experts)
        mine = lax.all_to_all(table, 'ep', 1, 0, tiled=True).reshape(-1, local_experts)
        total = jnp.zeros(x_all.shape, jnp.float32)
        for e in range(local_experts):
            gate_act = jnp.dot(x_all, wg_loc[e], preferred_element_type=jnp.float32)
            up_act = jnp.dot(x_all, wu_loc[e], preferred_element_type=jnp.float32)
            hidden = (jax.nn.silu(gate_act) * up_act).astype(jnp.bfloat16)
            out = jnp.dot(hidden, wd_loc[e], preferred_element_type=jnp.float32).astype(jnp.bfloat16)
            weight = mine[:, e:e + 1]
            total = total + jnp.where(weight != 0, weight * out.astype(jnp.float32), 0.0)
        return lax.psum_scatter(total, 'ep', scatter_dimension=0, tiled=True).astype(jnp.bfloat16)

    return jax.shard_map(local_layer, mesh=mesh,
                         in_specs=(row_spec, row_spec, row_spec, list_spec, list_spec, expert_spec, expert_spec, expert_spec),
                         out_specs=row_spec, check_vma=False)
```

```python
import functools

import jax
import jax.numpy as jnp
from jax import lax
from jax.experimental import pallas as pl
from jax.experimental.pallas import tpu as pltpu
from jax.sharding import PartitionSpec as P

CHIPS = 4
QUARTERS = 4
LANES = 8


def gate_table(ids_loc, gates_loc, hot_loc, hot_g_loc, group_size, local_experts):
    num_tokens = ids_loc.shape[0]
    slot = jnp.arange(group_size * LANES, dtype=jnp.int32)
    local = slot % LANES
    expert = jnp.where(local < local_experts, (slot // LANES) * local_experts + local, -1)
    token = jnp.arange(num_tokens, dtype=jnp.int32)
    cold = jnp.sum(jnp.where(ids_loc.T[:, None, :] == expert[None, :, None], gates_loc.T[:, None, :], 0.0), axis=0)
    hot = jnp.sum(jnp.where(hot_loc[:, None] == token[None, :], hot_g_loc[:, None], 0.0), axis=0)
    table = jnp.where(expert[:, None] == 0, hot[None, :], cold)
    return table.reshape(group_size, LANES, num_tokens)


def moe_kernel(x_hbm, tab_ref, wg_hbm, wu_hbm, wd_hbm, out_hbm,
               xall, wg, wu, wd, part, mate, ring, from_right, from_left, tabs, gcol, stage,
               w_sem, x_sem, ag_send, ag_recv, md_send, md_recv, tb_send, tb_recv,
               pd_send, pd_recv, rs_send, rs_recv, out_sem):
    experts = wg.shape[0]
    rows = xall.shape[2] // QUARTERS
    me = lax.axis_index('ep')
    chip, core = me // 2, me % 2
    right = ((chip + 1) % CHIPS) * 2 + core
    left = ((chip + CHIPS - 1) % CHIPS) * 2 + core
    partner = chip * 2 + (1 - core)

    def piece(p):
        return pl.ds(p * rows, rows)

    def remote(src, dst, send, recv, device):
        return pltpu.make_async_remote_copy(src_ref=src, dst_ref=dst, send_sem=send, recv_sem=recv,
                                            device_id={'ep': device}, device_id_type=pl.DeviceIdType.MESH)

    sends = []

    def start(make):
        make().start()
        sends.append(make)

    x_copy = pltpu.make_async_copy(x_hbm, xall.at[0, 0], x_sem)
    x_copy.start()
    w_copies = []
    for e in range(experts):
        for i, (src, dst) in enumerate(((wg_hbm, wg), (wu_hbm, wu), (wd_hbm, wd))):
            w_copies.append(pltpu.make_async_copy(src.at[e], dst.at[e], w_sem.at[3 * e + i]))
    for copy in w_copies:
        copy.start()

    barrier = pltpu.get_barrier_semaphore()
    peers = [(((chip + o) % CHIPS) * 2 + (core + q) % 2, o, q) for o in range(CHIPS) for q in range(2) if o or q]
    for device, _, _ in peers:
        pl.semaphore_signal(barrier, inc=1, device_id={'ep': device}, device_id_type=pl.DeviceIdType.MESH)
    pl.semaphore_wait(barrier, len(peers))

    def ring_send(o_src, o_dst, p, device):
        start(lambda: remote(xall.at[o_src, 0, piece(p)], xall.at[o_dst, 0, piece(p)],
                             ag_send.at[o_dst, p], ag_recv.at[o_dst, p], device))

    def mate_send(o, p):
        start(lambda: remote(xall.at[o, 0, piece(p)], xall.at[o, 1, piece(p)],
                             md_send.at[o, p], md_recv.at[o, p], partner))

    def ring_arrived(o, p):
        remote(xall.at[o, 0, piece(p)], xall.at[o, 0, piece(p)],
               ag_send.at[o, p], ag_recv.at[o, p], right).wait_recv()
        mate_send(o, p)

    def mate_arrived(o, p):
        remote(xall.at[o, 1, piece(p)], xall.at[o, 1, piece(p)],
               md_send.at[o, p], md_recv.at[o, p], partner).wait_recv()

    x_copy.wait()
    for p in (0, 1):
        ring_send(0, 3, p, right)
        ring_send(0, 1, p + 2, left)
    for p in range(QUARTERS):
        mate_send(0, p)
    for device, o, q in peers:
        start(functools.partial(remote, tab_ref.at[device], tabs.at[(CHIPS - o) % CHIPS, q], tb_send.at[o, q],
                                tb_recv.at[(CHIPS - o) % CHIPS, q], device))
    tabs[0, 0] = tab_ref[me]

    lane = lax.broadcasted_iota(jnp.int32, (rows, LANES), 1)

    def gates_ready(o, q):
        if o or q:
            remote(tabs.at[o, q], tabs.at[o, q], tb_send.at[o, q], tb_recv.at[o, q], partner).wait_recv()
        gcol[o, q] = jnp.transpose(tabs[o, q])

    def run_chunk(pairs, hooks, wait_weights):
        groups = [(o, q, p) for o, p in pairs for q in range(2)]
        for o, q, p in groups:
            part[o, q, piece(p)] = jnp.zeros((rows, part.shape[3]), jnp.float32)

        def body(e, _):
            for step, hook in hooks:
                pl.when(e == step)(hook)
            if wait_weights:
                for i in range(3):
                    ref = (wg, wu, wd)[i]
                    pltpu.make_async_copy(ref.at[e], ref.at[e], w_sem.at[3 * e + i]).wait()
            x = jnp.concatenate([xall[o, q, piece(p)] for o, q, p in groups], axis=0)
            half = wg.shape[2] // 2
            hidden = []
            for n in range(2):
                cols = pl.ds(n * half, half)
                a = jnp.dot(x, wg[e, :, cols], preferred_element_type=jnp.float32)
                b = jnp.dot(x, wu[e, :, cols], preferred_element_type=jnp.float32)
                hidden.append((a * jax.nn.sigmoid(a) * b).astype(jnp.bfloat16))
            u = jnp.concatenate(hidden, axis=1)
            weight = [jnp.sum(jnp.where(lane == e, gcol[o, q, piece(p)], 0.0), axis=1, keepdims=True)
                      for o, q, p in groups]
            width = 512
            for n in range(wd.shape[2] // width):
                cols = pl.ds(n * width, width)
                h = jnp.dot(u, wd[e, :, cols], preferred_element_type=jnp.float32).astype(jnp.bfloat16).astype(jnp.float32)
                for i, (o, q, p) in enumerate(groups):
                    hi = h[i * rows:(i + 1) * rows]
                    part[o, q, piece(p), cols] += jnp.where(weight[i] != 0, weight[i] * hi, 0.0)
            return 0

        lax.fori_loop(0, experts, body, 0)
        for o, p in pairs:
            start(functools.partial(remote, part.at[o, 1, piece(p)], mate.at[o, piece(p)],
                                    pd_send.at[o, p], pd_recv.at[o, p], partner))

    def partner_sum(o, p):
        remote(mate.at[o, piece(p)], mate.at[o, piece(p)], pd_send.at[o, p], pd_recv.at[o, p], partner).wait_recv()
        return part[o, 0, piece(p)] + mate[o, piece(p)]

    def rs_transfer(o, p, device):
        dst = {2: ring, 3: from_right, 1: from_left}[o]
        return remote(part.at[o, 0, piece(p)], dst.at[piece(p)], rs_send.at[o, p], rs_recv.at[o, p], device)

    def finish(o, p):
        total = partner_sum(o, p)
        goes_left = o == 3 or (o == 2 and p < 2)
        if (o == 3 and p < 2) or (o == 1 and p >= 2):
            rs_transfer(2, p, left).wait_recv()
            total = total + ring[piece(p)]
        part[o, 0, piece(p)] = total
        start(functools.partial(rs_transfer, o, p, left if goes_left else right))

    def forward(i):
        ring_arrived(3, i)
        ring_send(3, 2, i, right)
        ring_arrived(1, i + 2)
        ring_send(1, 2, i + 2, left)

    def forward_last():
        forward(1)
        for p in (0, 1):
            ring_send(0, 3, p + 2, right)
            ring_send(0, 1, p, left)

    def far(i):
        ring_arrived(2, i)
        ring_arrived(2, i + 2)

    def near(i):
        ring_arrived(3, i + 2)
        ring_arrived(1, i)

    def both(o1, p1, o2, p2):
        def act():
            finish(o1, p1)
            finish(o2, p2)
        return act

    def mates(*items):
        for o, p in items:
            mate_arrived(o, p)

    gates_ready(0, 0)
    gates_ready(0, 1)
    mates(*[(0, p) for p in range(QUARTERS)])
    run_chunk([(0, 0), (0, 2)], [(4, lambda: forward(0))], True)
    run_chunk([(0, 1), (0, 3)], [(2, forward_last), (4, lambda: far(0))], False)
    gates_ready(2, 0)
    gates_ready(2, 1)
    mates((2, 0), (2, 2))
    run_chunk([(2, 0), (2, 2)], [(3, lambda: far(1))], False)
    mates((2, 1), (2, 3))
    run_chunk([(2, 1), (2, 3)], [(1, both(2, 0, 2, 2)), (3, lambda: near(0))], False)
    for o in (1, 3):
        for q in range(2):
            gates_ready(o, q)
    mates((3, 2), (1, 0))
    run_chunk([(3, 2), (1, 0)], [(1, both(2, 1, 2, 3)), (3, lambda: near(1))], False)
    mates((3, 3), (1, 1))
    run_chunk([(3, 3), (1, 1)], [(1, both(3, 2, 1, 0))], False)
    mates((3, 0), (1, 2))
    run_chunk([(3, 0), (1, 2)], [(1, both(3, 3, 1, 1))], False)
    mates((3, 1), (1, 3))
    run_chunk([(3, 1), (1, 3)], [(1, both(3, 0, 1, 2))], False)
    both(3, 1, 1, 3)()

    for p in range(QUARTERS):
        part[0, 0, piece(p)] = partner_sum(0, p)
    out_copies = []
    for p in (0, 2, 1, 3):
        rs_transfer(3, p, left).wait_recv()
        rs_transfer(1, p, left).wait_recv()
        total = part[0, 0, piece(p)] + from_right[piece(p)] + from_left[piece(p)]
        stage[piece(p)] = total.astype(stage.dtype)
        copy = pltpu.make_async_copy(stage.at[piece(p)], out_hbm.at[piece(p)], out_sem.at[p])
        copy.start()
        out_copies.append(copy)
    for make in sends:
        make().wait_send()
    for copy in out_copies:
        copy.wait()


def solution(mesh):
    group_size = mesh.shape['ep']
    row_spec = P(('dp', 'ep'), None)
    list_spec = P(('dp', 'ep'))
    expert_spec = P('ep', None, None)

    def local_layer(x_loc, ids_loc, gates_loc, hot_loc, hot_g_loc, wg_loc, wu_loc, wd_loc):
        experts, d_model, d_ff = wg_loc.shape
        tokens = x_loc.shape[0]
        table = gate_table(ids_loc, gates_loc, hot_loc, hot_g_loc, group_size, experts)
        any_spec = pl.BlockSpec(memory_space=pl.ANY)
        dma = pltpu.SemaphoreType.DMA
        f32, bf16 = jnp.float32, jnp.bfloat16
        return pl.pallas_call(
            moe_kernel,
            out_shape=jax.ShapeDtypeStruct(x_loc.shape, x_loc.dtype),
            in_specs=[any_spec, pl.BlockSpec(memory_space=pltpu.VMEM), any_spec, any_spec, any_spec],
            out_specs=any_spec,
            scratch_shapes=[
                pltpu.VMEM((CHIPS, 2, tokens, d_model), bf16),
                pltpu.VMEM((experts, d_model, d_ff), bf16),
                pltpu.VMEM((experts, d_model, d_ff), bf16),
                pltpu.VMEM((experts, d_ff, d_model), bf16),
                pltpu.VMEM((CHIPS, 2, tokens, d_model), f32),
                pltpu.VMEM((CHIPS, tokens, d_model), f32),
                pltpu.VMEM((tokens, d_model), f32),
                pltpu.VMEM((tokens, d_model), f32),
                pltpu.VMEM((tokens, d_model), f32),
                pltpu.VMEM((CHIPS, 2, LANES, tokens), f32),
                pltpu.VMEM((CHIPS, 2, tokens, LANES), f32),
                pltpu.VMEM((tokens, d_model), bf16),
                dma((3 * experts,)), dma,
                dma((CHIPS, QUARTERS)), dma((CHIPS, QUARTERS)),
                dma((CHIPS, QUARTERS)), dma((CHIPS, QUARTERS)),
                dma((CHIPS, 2)), dma((CHIPS, 2)),
                dma((CHIPS, QUARTERS)), dma((CHIPS, QUARTERS)),
                dma((CHIPS, QUARTERS)), dma((CHIPS, QUARTERS)),
                dma((QUARTERS,)),
            ],
            compiler_params=pltpu.CompilerParams(collective_id=0, has_side_effects=True, vmem_limit_bytes=67_043_328),
            cost_estimate=pl.CostEstimate(flops=100_000_000, bytes_accessed=30_000_000, transcendentals=0),
            name='moe_ring',
        )(x_loc, table, wg_loc, wu_loc, wd_loc)

    return jax.shard_map(local_layer, mesh=mesh,
                         in_specs=(row_spec, row_spec, row_spec, list_spec, list_spec, expert_spec, expert_spec, expert_spec),
                         out_specs=row_spec, check_vma=False)
```

```python
import functools

import jax
import jax.numpy as jnp
from jax import lax
from jax.experimental import pallas as pl
from jax.experimental.pallas import tpu as pltpu
from jax.sharding import PartitionSpec as P

CHIPS = 4
QUARTERS = 4
LANES = 8


def build_table(ids, gates, hot_ref, hot_g_ref, tab_ref, experts):
    devices, padded, tokens = tab_ref.shape
    token_ids, token_gates = ids[...], gates[...]
    slot = lax.broadcasted_iota(jnp.int32, (padded, tokens), 0)
    token = lax.broadcasted_iota(jnp.int32, (1, tokens), 1)

    def add_hot(r, row):
        return jnp.where(token == hot_ref[r], hot_g_ref[r], row)

    hot = lax.fori_loop(0, hot_ref.shape[0], add_hot, jnp.zeros((1, tokens), jnp.float32), unroll=8)
    for d in range(devices):
        expert = jnp.where(slot < experts, d * experts + slot, -1)
        table = jnp.zeros((padded, tokens), jnp.float32)
        for j in range(token_ids.shape[0]):
            table = jnp.where(token_ids[j:j + 1] == expert, token_gates[j:j + 1], table)
        tab_ref[d] = jnp.where(expert == 0, hot, table)


def moe_kernel(hot_ref, hot_g_ref, x_hbm, ids_hbm, gates_hbm, wg_hbm, wu_hbm, wd_hbm, out_hbm,
               ids, gates, tab_ref, xall, wg, wu, wd, part, mate, ring, from_right, from_left, tabs, gcol, stage,
               w_sem, x_sem, in_sem, ag_send, ag_recv, md_send, md_recv, tb_send, tb_recv,
               pd_send, pd_recv, rs_send, rs_recv, out_sem):
    experts = wg.shape[0]
    rows = xall.shape[2] // QUARTERS
    me = lax.axis_index('ep')
    chip, core = me // 2, me % 2
    right = ((chip + 1) % CHIPS) * 2 + core
    left = ((chip + CHIPS - 1) % CHIPS) * 2 + core
    partner = chip * 2 + (1 - core)

    def piece(p):
        return pl.ds(p * rows, rows)

    def remote(src, dst, send, recv, device):
        return pltpu.make_async_remote_copy(src_ref=src, dst_ref=dst, send_sem=send, recv_sem=recv,
                                            device_id={'ep': device}, device_id_type=pl.DeviceIdType.MESH)

    sends = []

    def start(make):
        make().start()
        sends.append(make)

    x_copy = pltpu.make_async_copy(x_hbm, xall.at[0, 0], x_sem)
    x_copy.start()
    w_copies = []
    for e in range(experts):
        for i, (src, dst) in enumerate(((wg_hbm, wg), (wu_hbm, wu), (wd_hbm, wd))):
            w_copies.append(pltpu.make_async_copy(src.at[e], dst.at[e], w_sem.at[3 * e + i]))
    in_copies = [pltpu.make_async_copy(ids_hbm, ids, in_sem.at[0]), pltpu.make_async_copy(gates_hbm, gates, in_sem.at[1])]
    for copy in in_copies:
        copy.start()

    barrier = pltpu.get_barrier_semaphore()
    peers = [(((chip + o) % CHIPS) * 2 + (core + q) % 2, o, q) for o in range(CHIPS) for q in range(2) if o or q]
    for device, _, _ in peers:
        pl.semaphore_signal(barrier, inc=1, device_id={'ep': device}, device_id_type=pl.DeviceIdType.MESH)
    pl.semaphore_wait(barrier, len(peers))

    def ring_send(o_src, o_dst, p, device):
        start(lambda: remote(xall.at[o_src, 0, piece(p)], xall.at[o_dst, 0, piece(p)],
                             ag_send.at[o_dst, p], ag_recv.at[o_dst, p], device))

    def mate_send(o, p):
        start(lambda: remote(xall.at[o, 0, piece(p)], xall.at[o, 1, piece(p)],
                             md_send.at[o, p], md_recv.at[o, p], partner))

    def ring_arrived(o, p):
        remote(xall.at[o, 0, piece(p)], xall.at[o, 0, piece(p)],
               ag_send.at[o, p], ag_recv.at[o, p], right).wait_recv()
        mate_send(o, p)

    def mate_arrived(o, p):
        remote(xall.at[o, 1, piece(p)], xall.at[o, 1, piece(p)],
               md_send.at[o, p], md_recv.at[o, p], partner).wait_recv()

    x_copy.wait()
    for p in (0, 1):
        ring_send(0, 3, p, right)
        ring_send(0, 1, p + 2, left)
    for p in range(QUARTERS):
        mate_send(0, p)
    for copy in w_copies:
        copy.start()
    for copy in in_copies:
        copy.wait()
    build_table(ids, gates, hot_ref, hot_g_ref, tab_ref, experts)
    for device, o, q in peers:
        start(functools.partial(remote, tab_ref.at[device], tabs.at[(CHIPS - o) % CHIPS, q], tb_send.at[o, q],
                                tb_recv.at[(CHIPS - o) % CHIPS, q], device))
    tabs[0, 0] = tab_ref[me]

    lane = lax.broadcasted_iota(jnp.int32, (rows, LANES), 1)

    def gates_ready(o, q):
        if o or q:
            remote(tabs.at[o, q], tabs.at[o, q], tb_send.at[o, q], tb_recv.at[o, q], partner).wait_recv()
        gcol[o, q] = jnp.transpose(tabs[o, q])

    def run_chunk(pairs, first, last, hooks):
        groups = [(o, q, p) for o, p in pairs for q in range(2)]
        if first == 0:
            for o, q, p in groups:
                part[o, q, piece(p)] = jnp.zeros((rows, part.shape[3]), jnp.float32)

        def body(e, _):
            for step, hook in hooks:
                pl.when(e == step)(hook)
            if (pairs, first) == ([(0, 0), (0, 2)], 0):
                for i in range(3):
                    ref = (wg, wu, wd)[i]
                    pltpu.make_async_copy(ref.at[e], ref.at[e], w_sem.at[3 * e + i]).wait()
            x = jnp.concatenate([xall[o, q, piece(p)] for o, q, p in groups], axis=0)
            half = wg.shape[2] // 2
            hidden = []
            for n in range(2):
                cols = pl.ds(n * half, half)
                a = jnp.dot(x, wg[e, :, cols], preferred_element_type=jnp.float32)
                b = jnp.dot(x, wu[e, :, cols], preferred_element_type=jnp.float32)
                hidden.append((a * jax.nn.sigmoid(a) * b).astype(jnp.bfloat16))
            u = jnp.concatenate(hidden, axis=1)
            weight = [jnp.sum(jnp.where(lane == e, gcol[o, q, piece(p)], 0.0), axis=1, keepdims=True)
                      for o, q, p in groups]
            width = 512
            for n in range(wd.shape[2] // width):
                cols = pl.ds(n * width, width)
                h = jnp.dot(u, wd[e, :, cols], preferred_element_type=jnp.float32).astype(jnp.bfloat16).astype(jnp.float32)
                for i, (o, q, p) in enumerate(groups):
                    hi = h[i * rows:(i + 1) * rows]
                    part[o, q, piece(p), cols] += jnp.where(weight[i] != 0, weight[i] * hi, 0.0)
            return 0

        lax.fori_loop(first, last, body, 0)
        for o, p in pairs if last == experts else ():
            start(functools.partial(remote, part.at[o, 1, piece(p)], mate.at[o, piece(p)],
                                    pd_send.at[o, p], pd_recv.at[o, p], partner))

    def partner_sum(o, p):
        remote(mate.at[o, piece(p)], mate.at[o, piece(p)], pd_send.at[o, p], pd_recv.at[o, p], partner).wait_recv()
        return part[o, 0, piece(p)] + mate[o, piece(p)]

    def rs_transfer(o, p, device):
        dst = {2: ring, 3: from_right, 1: from_left}[o]
        return remote(part.at[o, 0, piece(p)], dst.at[piece(p)], rs_send.at[o, p], rs_recv.at[o, p], device)

    def finish(o, p):
        total = partner_sum(o, p)
        goes_left = o == 3 or (o == 2 and p < 2)
        if (o == 3 and p < 2) or (o == 1 and p >= 2):
            rs_transfer(2, p, left).wait_recv()
            total = total + ring[piece(p)]
        part[o, 0, piece(p)] = total
        start(functools.partial(rs_transfer, o, p, left if goes_left else right))

    def forward(i):
        ring_arrived(3, i)
        ring_send(3, 2, i, right)
        ring_arrived(1, i + 2)
        ring_send(1, 2, i + 2, left)

    def forward_last():
        forward(1)
        for p in (0, 1):
            ring_send(0, 3, p + 2, right)
            ring_send(0, 1, p, left)

    def far(i):
        ring_arrived(2, i)
        ring_arrived(2, i + 2)

    def near(i):
        ring_arrived(3, i + 2)
        ring_arrived(1, i)

    def both(o1, p1, o2, p2):
        def act():
            finish(o1, p1)
            finish(o2, p2)
        return act

    def mates(*items):
        for o, p in items:
            mate_arrived(o, p)

    gates_ready(0, 0)
    gates_ready(0, 1)
    mates(*[(0, p) for p in range(QUARTERS)])
    run_chunk([(0, 0), (0, 2)], 0, experts, [(2, lambda: forward(0)), (4, forward_last)])
    run_chunk([(0, 1), (0, 3)], 0, 3, [(2, lambda: far(0))])
    for q in range(2):
        gates_ready(2, q)
    mates((2, 0), (2, 2))
    run_chunk([(2, 0), (2, 2)], 0, experts, [(2, lambda: far(1)), (4, lambda: near(0))])
    mates((2, 1), (2, 3))
    run_chunk([(2, 1), (2, 3)], 0, experts, [(1, both(2, 0, 2, 2)), (3, lambda: near(1))])
    for o in (1, 3):
        for q in range(2):
            gates_ready(o, q)
    mates((3, 2), (1, 0))
    run_chunk([(3, 2), (1, 0)], 0, experts, [(1, both(2, 1, 2, 3))])
    mates((3, 3), (1, 1))
    run_chunk([(3, 3), (1, 1)], 0, experts, [(1, both(3, 2, 1, 0))])
    mates((3, 0), (1, 2))
    run_chunk([(3, 0), (1, 2)], 0, experts, [(1, both(3, 3, 1, 1))])
    mates((3, 1), (1, 3))
    run_chunk([(3, 1), (1, 3)], 0, experts, [(1, both(3, 0, 1, 2))])
    run_chunk([(0, 1), (0, 3)], 3, experts, [(3, both(3, 1, 1, 3))])

    for p in range(QUARTERS):
        part[0, 0, piece(p)] = partner_sum(0, p)
    out_copies = []
    for p in (0, 2, 1, 3):
        rs_transfer(3, p, left).wait_recv()
        rs_transfer(1, p, left).wait_recv()
        total = part[0, 0, piece(p)] + from_right[piece(p)] + from_left[piece(p)]
        stage[piece(p)] = total.astype(stage.dtype)
        copy = pltpu.make_async_copy(stage.at[piece(p)], out_hbm.at[piece(p)], out_sem.at[p])
        copy.start()
        out_copies.append(copy)
    for make in sends:
        make().wait_send()
    for copy in out_copies:
        copy.wait()


def solution(mesh):
    group_size = mesh.shape['ep']
    row_spec = P(('dp', 'ep'), None)
    list_spec = P(('dp', 'ep'))
    expert_spec = P('ep', None, None)

    def local_layer(x_loc, ids_loc, gates_loc, hot_loc, hot_g_loc, wg_loc, wu_loc, wd_loc):
        experts, d_model, d_ff = wg_loc.shape
        tokens = x_loc.shape[0]
        top_k = ids_loc.shape[1]
        smem_spec = pl.BlockSpec(memory_space=pltpu.SMEM)
        any_spec = pl.BlockSpec(memory_space=pl.ANY)
        dma = pltpu.SemaphoreType.DMA
        f32, bf16 = jnp.float32, jnp.bfloat16
        return pl.pallas_call(
            moe_kernel,
            out_shape=jax.ShapeDtypeStruct(x_loc.shape, x_loc.dtype),
            in_specs=[smem_spec, smem_spec] + [any_spec] * 6,
            out_specs=any_spec,
            scratch_shapes=[
                pltpu.VMEM((top_k, tokens), jnp.int32),
                pltpu.VMEM((top_k, tokens), f32),
                pltpu.VMEM((group_size, LANES, tokens), f32),
                pltpu.VMEM((CHIPS, 2, tokens, d_model), bf16),
                pltpu.VMEM((experts, d_model, d_ff), bf16),
                pltpu.VMEM((experts, d_model, d_ff), bf16),
                pltpu.VMEM((experts, d_ff, d_model), bf16),
                pltpu.VMEM((CHIPS, 2, tokens, d_model), f32),
                pltpu.VMEM((CHIPS, tokens, d_model), f32),
                pltpu.VMEM((tokens, d_model), f32),
                pltpu.VMEM((tokens, d_model), f32),
                pltpu.VMEM((tokens, d_model), f32),
                pltpu.VMEM((CHIPS, 2, LANES, tokens), f32),
                pltpu.VMEM((CHIPS, 2, tokens, LANES), f32),
                pltpu.VMEM((tokens, d_model), bf16),
                dma((3 * experts,)), dma, dma((2,)),
                dma((CHIPS, QUARTERS)), dma((CHIPS, QUARTERS)),
                dma((CHIPS, QUARTERS)), dma((CHIPS, QUARTERS)),
                dma((CHIPS, 2)), dma((CHIPS, 2)),
                dma((CHIPS, QUARTERS)), dma((CHIPS, QUARTERS)),
                dma((CHIPS, QUARTERS)), dma((CHIPS, QUARTERS)),
                dma((QUARTERS,)),
            ],
            compiler_params=pltpu.CompilerParams(collective_id=0, has_side_effects=True, vmem_limit_bytes=67_043_328),
            cost_estimate=pl.CostEstimate(flops=100_000_000, bytes_accessed=30_000_000, transcendentals=0),
            name='moe_ring',
        )(hot_loc, hot_g_loc, x_loc, ids_loc.T, gates_loc.T, wg_loc, wu_loc, wd_loc)

    return jax.shard_map(local_layer, mesh=mesh,
                         in_specs=(row_spec, row_spec, row_spec, list_spec, list_spec, expert_spec, expert_spec, expert_spec),
                         out_specs=row_spec, check_vma=False)
```

```python
import functools

import jax
import jax.numpy as jnp
from jax import lax
from jax.experimental import pallas as pl
from jax.experimental.pallas import tpu as pltpu
from jax.sharding import PartitionSpec as P

CHIPS = 4
QUARTERS = 4
STRIPS = 8
LANES = 8


def build_table(ids, gates, hot_ref, hot_g_ref, tab_ref, experts):
    devices, padded, tokens = tab_ref.shape
    token_ids, token_gates = ids[...], gates[...]
    slot = lax.broadcasted_iota(jnp.int32, (padded, tokens), 0)
    token = lax.broadcasted_iota(jnp.int32, (1, tokens), 1)

    def add_hot(r, row):
        return jnp.where(token == hot_ref[r], hot_g_ref[r], row)

    hot = lax.fori_loop(0, hot_ref.shape[0], add_hot, jnp.zeros((1, tokens), jnp.float32), unroll=8)
    for d in range(devices):
        expert = jnp.where(slot < experts, d * experts + slot, -1)
        table = jnp.zeros((padded, tokens), jnp.float32)
        for j in range(token_ids.shape[0]):
            table = jnp.where(token_ids[j:j + 1] == expert, token_gates[j:j + 1], table)
        tab_ref[d] = jnp.where(expert == 0, hot, table)


def moe_kernel(hot_hbm, hot_g_hbm, x_hbm, ids_hbm, gates_hbm, wg_hbm, wu_hbm, wd_hbm, out_hbm,
               hot_ref, hot_g_ref, ids, gates, tab_ref, xall, wg, wu, wd, part, mate, ring, from_right, from_left, tabs, gcol,
               w_sem, x_sem, in_sem, ag_send, ag_recv, md_send, md_recv, tb_send, tb_recv,
               pd_send, pd_recv, rs_send, rs_recv):
    experts = wg.shape[0]
    rows = xall.shape[2] // QUARTERS
    me = lax.axis_index('ep')
    chip, core = me // 2, me % 2
    right = ((chip + 1) % CHIPS) * 2 + core
    left = ((chip + CHIPS - 1) % CHIPS) * 2 + core
    partner = chip * 2 + (1 - core)

    def piece(p):
        return pl.ds(p * rows, rows)

    def strip(i):
        return pl.ds(i * (rows // 2), rows // 2)

    def remote(src, dst, send, recv, device):
        return pltpu.make_async_remote_copy(src_ref=src, dst_ref=dst, send_sem=send, recv_sem=recv,
                                            device_id={'ep': device}, device_id_type=pl.DeviceIdType.MESH)

    sends = []

    def start(make):
        make().start()
        sends.append(make)

    x_copies = [pltpu.make_async_copy(x_hbm.at[strip(i)], xall.at[0, 0, strip(i)], x_sem.at[i])
                for i in (0, 4, 1, 5, 2, 3, 6, 7)]
    for copy in x_copies:
        copy.start()
    w_copies = []
    for e in range(experts):
        for i, (src, dst) in enumerate(((wg_hbm, wg), (wu_hbm, wu), (wd_hbm, wd))):
            w_copies.append(pltpu.make_async_copy(src.at[e], dst.at[e], w_sem.at[3 * e + i]))
    in_copies = [pltpu.make_async_copy(ids_hbm, ids, in_sem.at[0]), pltpu.make_async_copy(gates_hbm, gates, in_sem.at[1]),
                 pltpu.make_async_copy(hot_hbm, hot_ref, in_sem.at[2]), pltpu.make_async_copy(hot_g_hbm, hot_g_ref, in_sem.at[3])]
    for copy in in_copies:
        copy.start()

    barrier = pltpu.get_barrier_semaphore()
    peers = [(((chip + o) % CHIPS) * 2 + (core + q) % 2, o, q) for o in range(CHIPS) for q in range(2) if o or q]
    for device, _, _ in peers:
        pl.semaphore_signal(barrier, inc=1, device_id={'ep': device}, device_id_type=pl.DeviceIdType.MESH)
    pl.semaphore_wait(barrier, len(peers))

    def ring_send(o_src, o_dst, s, device):
        start(lambda: remote(xall.at[o_src, 0, strip(s)], xall.at[o_dst, 0, strip(s)],
                             ag_send.at[o_dst, s], ag_recv.at[o_dst, s], device))

    def mate_send(o, s):
        start(lambda: remote(xall.at[o, 0, strip(s)], xall.at[o, 1, strip(s)],
                             md_send.at[o, s], md_recv.at[o, s], partner))

    def ring_arrived(o, s):
        remote(xall.at[o, 0, strip(s)], xall.at[o, 0, strip(s)],
               ag_send.at[o, s], ag_recv.at[o, s], right).wait_recv()
        mate_send(o, s)

    def mate_arrived(o, p):
        for s in (2 * p, 2 * p + 1):
            remote(xall.at[o, 1, strip(s)], xall.at[o, 1, strip(s)],
                   md_send.at[o, s], md_recv.at[o, s], partner).wait_recv()

    for i in (0, 1):
        x_copies[2 * i].wait()
        ring_send(0, 3, i, right)
        x_copies[2 * i + 1].wait()
        ring_send(0, 1, i + 4, left)
    for copy in x_copies[4:]:
        copy.wait()
    for i in range(STRIPS):
        mate_send(0, i)
    for copy in w_copies:
        copy.start()
    for copy in in_copies:
        copy.wait()
    build_table(ids, gates, hot_ref, hot_g_ref, tab_ref, experts)
    for device, o, q in peers:
        start(functools.partial(remote, tab_ref.at[device, pl.ds(0, experts)],
                                tabs.at[(CHIPS - o) % CHIPS, q, pl.ds(0, experts)], tb_send.at[o, q],
                                tb_recv.at[(CHIPS - o) % CHIPS, q], device))
    tabs[0, 0] = tab_ref[me]

    lane = lax.broadcasted_iota(jnp.int32, (rows, LANES), 1)

    def gates_ready(o, q):
        if o or q:
            remote(tabs.at[o, q, pl.ds(0, experts)], tabs.at[o, q, pl.ds(0, experts)], tb_send.at[o, q], tb_recv.at[o, q], partner).wait_recv()
        gcol[o, q] = jnp.transpose(tabs[o, q])

    def run_chunk(pairs, first, last, hooks):
        groups = [(o, q, p) for o, p in pairs for q in range(2)]
        if first == 0:
            for o, q, p in groups:
                part[o, q, piece(p)] = jnp.zeros((rows, part.shape[3]), jnp.float32)

        def body(e, _):
            for step, hook in hooks:
                pl.when(e == step)(hook)
            if (pairs, first) == ([(0, 0), (0, 2)], 0):
                for i in range(3):
                    ref = (wg, wu, wd)[i]
                    pltpu.make_async_copy(ref.at[e], ref.at[e], w_sem.at[3 * e + i]).wait()
            x = jnp.concatenate([xall[o, q, piece(p)] for o, q, p in groups], axis=0)
            half = wg.shape[2] // 2
            hidden = []
            for n in range(2):
                cols = pl.ds(n * half, half)
                a = jnp.dot(x, wg[e, :, cols], preferred_element_type=jnp.float32)
                b = jnp.dot(x, wu[e, :, cols], preferred_element_type=jnp.float32)
                hidden.append((a * jax.nn.sigmoid(a) * b).astype(jnp.bfloat16))
            u = jnp.concatenate(hidden, axis=1)
            weight = [jnp.sum(jnp.where(lane == e, gcol[o, q, piece(p)], 0.0), axis=1, keepdims=True)
                      for o, q, p in groups]
            width = 512
            for n in range(wd.shape[2] // width):
                cols = pl.ds(n * width, width)
                h = jnp.dot(u, wd[e, :, cols], preferred_element_type=jnp.float32).astype(jnp.bfloat16).astype(jnp.float32)
                for i, (o, q, p) in enumerate(groups):
                    hi = h[i * rows:(i + 1) * rows]
                    part[o, q, piece(p), cols] += jnp.where(weight[i] != 0, weight[i] * hi, 0.0)
            return 0

        lax.fori_loop(first, last, body, 0)
        for o, p in pairs if last == experts else ():
            start(functools.partial(remote, part.at[o, 1, piece(p)], mate.at[o, piece(p)],
                                    pd_send.at[o, p], pd_recv.at[o, p], partner))

    def partner_sum(o, p):
        remote(mate.at[o, piece(p)], mate.at[o, piece(p)], pd_send.at[o, p], pd_recv.at[o, p], partner).wait_recv()
        return part[o, 0, piece(p)] + mate[o, piece(p)]

    def rs_transfer(o, p, device):
        dst = {2: ring, 3: from_right, 1: from_left}[o]
        return remote(part.at[o, 0, piece(p)], dst.at[piece(p)], rs_send.at[o, p], rs_recv.at[o, p], device)

    def finish(o, p):
        total = partner_sum(o, p)
        goes_left = o == 3 or (o == 2 and p < 2)
        if (o == 3 and p < 2) or (o == 1 and p >= 2):
            rs_transfer(2, p, left).wait_recv()
            total = total + ring[piece(p)]
        part[o, 0, piece(p)] = total
        start(functools.partial(rs_transfer, o, p, left if goes_left else right))

    def stage(i):
        def act():
            ring_arrived(3, i)
            ring_send(3, 2, i, right)
            ring_arrived(1, i + 4)
            ring_send(1, 2, i + 4, left)
            for own in ((2,), (3,), (4,), (5, 6, 7))[i]:
                ring_send(0, 3, own, right)
                ring_send(0, 1, (own + 4) % STRIPS, left)
        return act

    def far(i):
        def act():
            for s in (2 * i, 2 * i + 1, 2 * i + 4, 2 * i + 5):
                ring_arrived(2, s)
        return act

    def near(i):
        def act():
            for s in (2 * i, 2 * i + 1):
                ring_arrived(3, s + 4)
                ring_arrived(1, s)
        return act

    def both(o1, p1, o2, p2):
        def act():
            finish(o1, p1)
            finish(o2, p2)
        return act

    def mates(*items):
        for o, p in items:
            mate_arrived(o, p)

    gates_ready(0, 0)
    gates_ready(0, 1)
    mates(*[(0, p) for p in range(QUARTERS)])
    run_chunk([(0, 0), (0, 2)], 0, experts, [(1, stage(0)), (3, stage(1))])
    run_chunk([(0, 1), (0, 3)], 0, 3, [(1, stage(2)), (2, far(0))])
    for q in range(2):
        gates_ready(2, q)
    mates((2, 0), (2, 2))
    run_chunk([(2, 0), (2, 2)], 0, experts, [(1, stage(3)), (4, far(1))])
    mates((2, 1), (2, 3))
    run_chunk([(2, 1), (2, 3)], 0, experts, [(1, both(2, 0, 2, 2)), (3, near(0))])
    for o in (1, 3):
        for q in range(2):
            gates_ready(o, q)
    mates((3, 2), (1, 0))
    run_chunk([(3, 2), (1, 0)], 0, experts, [(1, both(2, 1, 2, 3)), (2, near(1))])
    mates((3, 3), (1, 1))
    run_chunk([(3, 3), (1, 1)], 0, experts, [(1, both(3, 2, 1, 0))])
    mates((3, 0), (1, 2))
    run_chunk([(3, 0), (1, 2)], 0, experts, [(1, both(3, 3, 1, 1))])
    mates((3, 1), (1, 3))
    run_chunk([(3, 1), (1, 3)], 0, experts, [(1, both(3, 0, 1, 2))])
    run_chunk([(0, 1), (0, 3)], 3, experts, [(4, both(3, 1, 1, 3))])

    for p in range(QUARTERS):
        part[0, 0, piece(p)] = partner_sum(0, p)
    out_copies = []
    for p in (0, 2, 1, 3):
        rs_transfer(3, p, left).wait_recv()
        rs_transfer(1, p, left).wait_recv()
        total = part[0, 0, piece(p)] + from_right[piece(p)] + from_left[piece(p)]
        out_hbm[piece(p)] = total.astype(out_hbm.dtype)
    for make in sends:
        make().wait_send()


def solution(mesh):
    group_size = mesh.shape['ep']
    row_spec = P(('dp', 'ep'), None)
    list_spec = P(('dp', 'ep'))
    expert_spec = P('ep', None, None)

    def local_layer(x_loc, ids_loc, gates_loc, hot_loc, hot_g_loc, wg_loc, wu_loc, wd_loc):
        experts, d_model, d_ff = wg_loc.shape
        tokens = x_loc.shape[0]
        top_k = ids_loc.shape[1]
        hot_rows = hot_loc.shape[0]
        any_spec = pl.BlockSpec(memory_space=pl.ANY)
        dma = pltpu.SemaphoreType.DMA
        f32, bf16 = jnp.float32, jnp.bfloat16
        return pl.pallas_call(
            moe_kernel,
            out_shape=pltpu.VMEM(x_loc.shape, x_loc.dtype),
            in_specs=[any_spec] * 8,
            out_specs=pl.BlockSpec(memory_space=pltpu.VMEM),
            scratch_shapes=[
                pltpu.SMEM((hot_rows,), jnp.int32),
                pltpu.SMEM((hot_rows,), f32),
                pltpu.VMEM((top_k, tokens), jnp.int32),
                pltpu.VMEM((top_k, tokens), f32),
                pltpu.VMEM((group_size, LANES, tokens), f32),
                pltpu.VMEM((CHIPS, 2, tokens, d_model), bf16),
                pltpu.VMEM((experts, d_model, d_ff), bf16),
                pltpu.VMEM((experts, d_model, d_ff), bf16),
                pltpu.VMEM((experts, d_ff, d_model), bf16),
                pltpu.VMEM((CHIPS, 2, tokens, d_model), f32),
                pltpu.VMEM((CHIPS, tokens, d_model), f32),
                pltpu.VMEM((tokens, d_model), f32),
                pltpu.VMEM((tokens, d_model), f32),
                pltpu.VMEM((tokens, d_model), f32),
                pltpu.VMEM((CHIPS, 2, LANES, tokens), f32),
                pltpu.VMEM((CHIPS, 2, tokens, LANES), f32),
                dma((3 * experts,)), dma((STRIPS,)), dma((4,)),
                dma((CHIPS, STRIPS)), dma((CHIPS, STRIPS)),
                dma((CHIPS, STRIPS)), dma((CHIPS, STRIPS)),
                dma((CHIPS, 2)), dma((CHIPS, 2)),
                dma((CHIPS, QUARTERS)), dma((CHIPS, QUARTERS)),
                dma((CHIPS, QUARTERS)), dma((CHIPS, QUARTERS)),
            ],
            compiler_params=pltpu.CompilerParams(collective_id=0, has_side_effects=True, vmem_limit_bytes=62_000_000),
            cost_estimate=pl.CostEstimate(flops=100_000_000, bytes_accessed=30_000_000, transcendentals=0),
            name='moe_ring',
        )(hot_loc, hot_g_loc, x_loc, ids_loc.T, gates_loc.T, wg_loc, wu_loc, wd_loc)

    return jax.shard_map(local_layer, mesh=mesh,
                         in_specs=(row_spec, row_spec, row_spec, list_spec, list_spec, expert_spec, expert_spec, expert_spec),
                         out_specs=row_spec, check_vma=False)
```

```python
import functools

import jax
import jax.numpy as jnp
from jax import lax
from jax.experimental import pallas as pl
from jax.experimental.pallas import tpu as pltpu
from jax.sharding import PartitionSpec as P

CHIPS = 4
QUARTERS = 4
STRIPS = 8
LANES = 8


def build_table(ids, gates, hot_ref, hot_g_ref, tab_ref, experts):
    devices, padded, tokens = tab_ref.shape
    token_ids, token_gates = ids[...], gates[...]
    slot = lax.broadcasted_iota(jnp.int32, (padded, tokens), 0)
    token = lax.broadcasted_iota(jnp.int32, (1, tokens), 1)

    def add_hot(r, row):
        return jnp.where(token == hot_ref[r], hot_g_ref[r], row)

    hot = lax.fori_loop(0, hot_ref.shape[0], add_hot, jnp.zeros((1, tokens), jnp.float32), unroll=8)
    for d in range(devices):
        expert = jnp.where(slot < experts, d * experts + slot, -1)
        table = jnp.zeros((padded, tokens), jnp.float32)
        for j in range(token_ids.shape[0]):
            table = jnp.where(token_ids[j:j + 1] == expert, token_gates[j:j + 1], table)
        tab_ref[d] = jnp.where(expert == 0, hot, table)


def moe_kernel(hot_hbm, hot_g_hbm, x_hbm, ids_hbm, gates_hbm, wg_hbm, wu_hbm, wd_hbm, out_hbm,
               hot_ref, hot_g_ref, ids, gates, tab_ref, xall, wg, wu, wd, part, mate, ring, from_right, from_left, tabs, gcol,
               w_sem, x_sem, in_sem, ag_send, ag_recv, md_send, md_recv, tb_send, tb_recv,
               pd_send, pd_recv, rs_send, rs_recv):
    experts = wg.shape[0]
    rows = xall.shape[2] // QUARTERS
    me = lax.axis_index('ep')
    chip, core = me // 2, me % 2
    right = ((chip + 1) % CHIPS) * 2 + core
    left = ((chip + CHIPS - 1) % CHIPS) * 2 + core
    partner = chip * 2 + (1 - core)

    def piece(p):
        return pl.ds(p * rows, rows)

    def strip(i):
        return pl.ds(i * (rows // 2), rows // 2)

    def remote(src, dst, send, recv, device):
        return pltpu.make_async_remote_copy(src_ref=src, dst_ref=dst, send_sem=send, recv_sem=recv,
                                            device_id={'ep': device}, device_id_type=pl.DeviceIdType.MESH)

    sends = []

    def start(make):
        make().start()
        sends.append(make)

    x_copies = [pltpu.make_async_copy(x_hbm.at[strip(i)], xall.at[0, 0, strip(i)], x_sem.at[i])
                for i in (0, 4, 1, 5, 2, 3, 6, 7)]
    for copy in x_copies:
        copy.start()
    w_copies = []
    for e in range(experts):
        for i, (src, dst) in enumerate(((wg_hbm, wg), (wu_hbm, wu), (wd_hbm, wd))):
            w_copies.append(pltpu.make_async_copy(src.at[e], dst.at[e], w_sem.at[3 * e + i]))
    in_copies = [pltpu.make_async_copy(ids_hbm, ids, in_sem.at[0]), pltpu.make_async_copy(gates_hbm, gates, in_sem.at[1]),
                 pltpu.make_async_copy(hot_hbm, hot_ref, in_sem.at[2]), pltpu.make_async_copy(hot_g_hbm, hot_g_ref, in_sem.at[3])]
    for copy in in_copies:
        copy.start()

    barrier = pltpu.get_barrier_semaphore()
    peers = [(((chip + o) % CHIPS) * 2 + (core + q) % 2, o, q) for o in range(CHIPS) for q in range(2) if o or q]
    for device, _, _ in peers:
        pl.semaphore_signal(barrier, inc=1, device_id={'ep': device}, device_id_type=pl.DeviceIdType.MESH)
    pl.semaphore_wait(barrier, len(peers))

    def ring_send(o_src, o_dst, s, device):
        start(lambda: remote(xall.at[o_src, 0, strip(s)], xall.at[o_dst, 0, strip(s)],
                             ag_send.at[o_dst, s], ag_recv.at[o_dst, s], device))

    def mate_send(o, s):
        start(lambda: remote(xall.at[o, 0, strip(s)], xall.at[o, 1, strip(s)],
                             md_send.at[o, s], md_recv.at[o, s], partner))

    def ring_arrived(o, s):
        remote(xall.at[o, 0, strip(s)], xall.at[o, 0, strip(s)],
               ag_send.at[o, s], ag_recv.at[o, s], right).wait_recv()
        mate_send(o, s)

    def mate_arrived(o, p):
        for s in (2 * p, 2 * p + 1):
            remote(xall.at[o, 1, strip(s)], xall.at[o, 1, strip(s)],
                   md_send.at[o, s], md_recv.at[o, s], partner).wait_recv()

    for i in (0, 1):
        x_copies[2 * i].wait()
        ring_send(0, 3, i, right)
        x_copies[2 * i + 1].wait()
        ring_send(0, 1, i + 4, left)
    for copy in x_copies[4:]:
        copy.wait()
    for i in range(STRIPS):
        mate_send(0, i)
    for copy in w_copies:
        copy.start()
    for copy in in_copies:
        copy.wait()
    build_table(ids, gates, hot_ref, hot_g_ref, tab_ref, experts)
    for device, o, q in peers:
        start(functools.partial(remote, tab_ref.at[device, pl.ds(0, experts)],
                                tabs.at[(CHIPS - o) % CHIPS, q, pl.ds(0, experts)], tb_send.at[o, q],
                                tb_recv.at[(CHIPS - o) % CHIPS, q], device))
    tabs[0, 0] = tab_ref[me]

    lane = lax.broadcasted_iota(jnp.int32, (rows, LANES), 1)

    def gates_ready(o, q):
        if o or q:
            remote(tabs.at[o, q, pl.ds(0, experts)], tabs.at[o, q, pl.ds(0, experts)], tb_send.at[o, q], tb_recv.at[o, q], partner).wait_recv()
        gcol[o, q] = jnp.transpose(tabs[o, q])

    def run_chunk(pairs, first, last, hooks, unroll=False):
        groups = [(o, q, p) for o, p in pairs for q in range(2)]
        if first == 0:
            for o, q, p in groups:
                part[o, q, piece(p)] = jnp.zeros((rows, part.shape[3]), jnp.float32)

        def call_hooks(at):
            for step, hook in hooks:
                if not unroll:
                    pl.when(at == step)(hook)
                elif at == step:
                    hook()

        def body(e, _):
            call_hooks(e)
            if (pairs, first) == ([(0, 0), (0, 2)], 0):
                for i in range(3):
                    ref = (wg, wu, wd)[i]
                    pltpu.make_async_copy(ref.at[e], ref.at[e], w_sem.at[3 * e + i]).wait()
            x = jnp.concatenate([xall[o, q, piece(p)] for o, q, p in groups], axis=0)
            half = wg.shape[2] // 2
            hidden = []
            for n in range(2):
                cols = pl.ds(n * half, half)
                a = jnp.dot(x, wg[e, :, cols], preferred_element_type=jnp.float32)
                b = jnp.dot(x, wu[e, :, cols], preferred_element_type=jnp.float32)
                hidden.append((a * jax.nn.sigmoid(a) * b).astype(jnp.bfloat16))
            if unroll:
                call_hooks(e + 0.5)
            u = jnp.concatenate(hidden, axis=1)
            weight = [jnp.sum(jnp.where(lane == e, gcol[o, q, piece(p)], 0.0), axis=1, keepdims=True)
                      for o, q, p in groups]
            width = 512
            for n in range(wd.shape[2] // width):
                cols = pl.ds(n * width, width)
                h = jnp.dot(u, wd[e, :, cols], preferred_element_type=jnp.float32).astype(jnp.bfloat16).astype(jnp.float32)
                for i, (o, q, p) in enumerate(groups):
                    hi = h[i * rows:(i + 1) * rows]
                    part[o, q, piece(p), cols] += jnp.where(weight[i] != 0, weight[i] * hi, 0.0)
            return 0

        if unroll:
            for e in range(first, last):
                body(e, 0)
        else:
            lax.fori_loop(first, last, body, 0)
        for o, p in pairs if last == experts else ():
            start(functools.partial(remote, part.at[o, 1, piece(p)], mate.at[o, piece(p)],
                                    pd_send.at[o, p], pd_recv.at[o, p], partner))

    def partner_sum(o, p):
        remote(mate.at[o, piece(p)], mate.at[o, piece(p)], pd_send.at[o, p], pd_recv.at[o, p], partner).wait_recv()
        return part[o, 0, piece(p)] + mate[o, piece(p)]

    def rs_transfer(o, p, device):
        dst = {2: ring, 3: from_right, 1: from_left}[o]
        return remote(part.at[o, 0, piece(p)], dst.at[piece(p)], rs_send.at[o, p], rs_recv.at[o, p], device)

    def finish(o, p):
        total = partner_sum(o, p)
        goes_left = o == 3 or (o == 2 and p < 2)
        if (o == 3 and p < 2) or (o == 1 and p >= 2):
            rs_transfer(2, p, left).wait_recv()
            total = total + ring[piece(p)]
        part[o, 0, piece(p)] = total
        start(functools.partial(rs_transfer, o, p, left if goes_left else right))

    def stage(i):
        def act():
            ring_arrived(3, i)
            ring_send(3, 2, i, right)
            ring_arrived(1, i + 4)
            ring_send(1, 2, i + 4, left)
            for own in ((2,), (3,), (4,), (5, 6, 7))[i]:
                ring_send(0, 3, own, right)
                ring_send(0, 1, (own + 4) % STRIPS, left)
        return act

    def far(i):
        def act():
            for s in (2 * i, 2 * i + 1, 2 * i + 4, 2 * i + 5):
                ring_arrived(2, s)
        return act

    def near(i):
        def act():
            for s in (2 * i, 2 * i + 1):
                ring_arrived(3, s + 4)
                ring_arrived(1, s)
        return act

    def both(o1, p1, o2, p2):
        def act():
            finish(o1, p1)
            finish(o2, p2)
        return act

    def mates(*items):
        for o, p in items:
            mate_arrived(o, p)

    gates_ready(0, 0)
    gates_ready(0, 1)
    mates(*[(0, p) for p in range(QUARTERS)])
    run_chunk([(0, 0), (0, 2)], 0, experts, [(1, stage(0)), (3, stage(1))])
    run_chunk([(0, 1), (0, 3)], 0, 2, [(1, stage(2))])
    far(0)()
    for q in range(2):
        gates_ready(2, q)
    mates((2, 0), (2, 2))
    run_chunk([(2, 0), (2, 2)], 0, experts, [(1, stage(3)), (4, far(1))], True)
    mates((2, 1), (2, 3))
    run_chunk([(2, 1), (2, 3)], 0, experts, [(1.5, both(2, 0, 2, 2)), (3, near(0))], True)
    for o in (1, 3):
        for q in range(2):
            gates_ready(o, q)
    mates((3, 2), (1, 0))
    run_chunk([(3, 2), (1, 0)], 0, experts, [(1.5, both(2, 1, 2, 3)), (2, near(1))], True)
    mates((3, 3), (1, 1))
    run_chunk([(3, 3), (1, 1)], 0, experts, [(1.5, both(3, 2, 1, 0))], True)
    mates((3, 0), (1, 2))
    run_chunk([(3, 0), (1, 2)], 0, experts, [(1.5, both(3, 3, 1, 1))], True)
    mates((3, 1), (1, 3))
    run_chunk([(3, 1), (1, 3)], 0, experts, [(1, both(3, 0, 1, 2))])
    run_chunk([(0, 1), (0, 3)], 2, experts, [(4, both(3, 1, 1, 3))])

    for p in range(QUARTERS):
        part[0, 0, piece(p)] = partner_sum(0, p)
    out_copies = []
    for p in (0, 2, 1, 3):
        rs_transfer(3, p, left).wait_recv()
        rs_transfer(1, p, left).wait_recv()
        total = part[0, 0, piece(p)] + from_right[piece(p)] + from_left[piece(p)]
        out_hbm[piece(p)] = total.astype(out_hbm.dtype)
    for make in sends:
        make().wait_send()


def solution(mesh):
    group_size = mesh.shape['ep']
    row_spec = P(('dp', 'ep'), None)
    list_spec = P(('dp', 'ep'))
    expert_spec = P('ep', None, None)

    def local_layer(x_loc, ids_loc, gates_loc, hot_loc, hot_g_loc, wg_loc, wu_loc, wd_loc):
        experts, d_model, d_ff = wg_loc.shape
        tokens = x_loc.shape[0]
        top_k = ids_loc.shape[1]
        hot_rows = hot_loc.shape[0]
        any_spec = pl.BlockSpec(memory_space=pl.ANY)
        dma = pltpu.SemaphoreType.DMA
        f32, bf16 = jnp.float32, jnp.bfloat16
        return pl.pallas_call(
            moe_kernel,
            out_shape=pltpu.VMEM(x_loc.shape, x_loc.dtype),
            in_specs=[any_spec] * 8,
            out_specs=pl.BlockSpec(memory_space=pltpu.VMEM),
            scratch_shapes=[
                pltpu.SMEM((hot_rows,), jnp.int32),
                pltpu.SMEM((hot_rows,), f32),
                pltpu.VMEM((top_k, tokens), jnp.int32),
                pltpu.VMEM((top_k, tokens), f32),
                pltpu.VMEM((group_size, LANES, tokens), f32),
                pltpu.VMEM((CHIPS, 2, tokens, d_model), bf16),
                pltpu.VMEM((experts, d_model, d_ff), bf16),
                pltpu.VMEM((experts, d_model, d_ff), bf16),
                pltpu.VMEM((experts, d_ff, d_model), bf16),
                pltpu.VMEM((CHIPS, 2, tokens, d_model), f32),
                pltpu.VMEM((CHIPS, tokens, d_model), f32),
                pltpu.VMEM((tokens, d_model), f32),
                pltpu.VMEM((tokens, d_model), f32),
                pltpu.VMEM((tokens, d_model), f32),
                pltpu.VMEM((CHIPS, 2, LANES, tokens), f32),
                pltpu.VMEM((CHIPS, 2, tokens, LANES), f32),
                dma((3 * experts,)), dma((STRIPS,)), dma((4,)),
                dma((CHIPS, STRIPS)), dma((CHIPS, STRIPS)),
                dma((CHIPS, STRIPS)), dma((CHIPS, STRIPS)),
                dma((CHIPS, 2)), dma((CHIPS, 2)),
                dma((CHIPS, QUARTERS)), dma((CHIPS, QUARTERS)),
                dma((CHIPS, QUARTERS)), dma((CHIPS, QUARTERS)),
            ],
            compiler_params=pltpu.CompilerParams(collective_id=0, has_side_effects=True, vmem_limit_bytes=62_000_000),
            cost_estimate=pl.CostEstimate(flops=100_000_000, bytes_accessed=30_000_000, transcendentals=0),
            name='moe_ring',
        )(hot_loc, hot_g_loc, x_loc, ids_loc.T, gates_loc.T, wg_loc, wu_loc, wd_loc)

    return jax.shard_map(local_layer, mesh=mesh,
                         in_specs=(row_spec, row_spec, row_spec, list_spec, list_spec, expert_spec, expert_spec, expert_spec),
                         out_specs=row_spec, check_vma=False)
```

```python
import functools

import jax
import jax.numpy as jnp
from jax import lax
from jax.experimental import pallas as pl
from jax.experimental.pallas import tpu as pltpu
from jax.sharding import PartitionSpec as P

CHIPS = 4
QUARTERS = 4
STRIPS = 8
LANES = 8


def build_table(ids, gates, hot_ref, hot_g_ref, tab_ref, experts):
    devices, padded, tokens = tab_ref.shape
    token_ids, token_gates = ids[...], gates[...]
    slot = lax.broadcasted_iota(jnp.int32, (padded, tokens), 0)
    token = lax.broadcasted_iota(jnp.int32, (1, tokens), 1)

    def add_hot(r, row):
        return jnp.where(token == hot_ref[r], hot_g_ref[r], row)

    hot = lax.fori_loop(0, hot_ref.shape[0], add_hot, jnp.zeros((1, tokens), jnp.float32), unroll=8)
    for d in range(devices):
        expert = jnp.where(slot < experts, d * experts + slot, -1)
        table = jnp.zeros((padded, tokens), jnp.float32)
        for j in range(token_ids.shape[0]):
            table = jnp.where(token_ids[j:j + 1] == expert, token_gates[j:j + 1], table)
        tab_ref[d] = jnp.where(expert == 0, hot, table)


def moe_kernel(hot_hbm, hot_g_hbm, x_hbm, ids_hbm, gates_hbm, wg_hbm, wu_hbm, wd_hbm, out_hbm,
               hot_ref, hot_g_ref, ids, gates, tab_ref, xall, wg, wu, wd, part, mate, ring, from_right, from_left, tabs, gcol,
               w_sem, x_sem, in_sem, ag_send, ag_recv, md_send, md_recv, tb_send, tb_recv,
               pd_send, pd_recv, rs_send, rs_recv):
    experts = wg.shape[0]
    rows = xall.shape[2] // QUARTERS
    me = lax.axis_index('ep')
    chip, core = me // 2, me % 2
    right = ((chip + 1) % CHIPS) * 2 + core
    left = ((chip + CHIPS - 1) % CHIPS) * 2 + core
    partner = chip * 2 + (1 - core)

    def piece(p):
        return pl.ds(p * rows, rows)

    def strip(i):
        return pl.ds(i * (rows // 2), rows // 2)

    def remote(src, dst, send, recv, device):
        return pltpu.make_async_remote_copy(src_ref=src, dst_ref=dst, send_sem=send, recv_sem=recv,
                                            device_id={'ep': device}, device_id_type=pl.DeviceIdType.MESH)

    sends, sums_sent = [], []

    def start(make):
        make().start()
        sends.append(make)

    x_copies = [pltpu.make_async_copy(x_hbm.at[strip(i)], xall.at[0, 0, strip(i)], x_sem.at[i])
                for i in (0, 4, 1, 5, 2, 3, 6, 7)]
    for copy in x_copies:
        copy.start()
    w_copies = []
    for e in range(experts):
        for i, (src, dst) in enumerate(((wg_hbm, wg), (wu_hbm, wu), (wd_hbm, wd))):
            w_copies.append(pltpu.make_async_copy(src.at[e], dst.at[e], w_sem.at[3 * e + i]))
    in_copies = [pltpu.make_async_copy(ids_hbm, ids, in_sem.at[0]), pltpu.make_async_copy(gates_hbm, gates, in_sem.at[1]),
                 pltpu.make_async_copy(hot_hbm, hot_ref, in_sem.at[2]), pltpu.make_async_copy(hot_g_hbm, hot_g_ref, in_sem.at[3])]
    for copy in in_copies:
        copy.start()

    barrier = pltpu.get_barrier_semaphore()
    peers = [(((chip + o) % CHIPS) * 2 + (core + q) % 2, o, q) for o in range(CHIPS) for q in range(2) if o or q]
    for device, _, _ in peers:
        pl.semaphore_signal(barrier, inc=1, device_id={'ep': device}, device_id_type=pl.DeviceIdType.MESH)
    pl.semaphore_wait(barrier, len(peers))

    def ring_send(o_src, o_dst, s, device):
        start(lambda: remote(xall.at[o_src, 0, strip(s)], xall.at[o_dst, 0, strip(s)],
                             ag_send.at[o_dst, s], ag_recv.at[o_dst, s], device))

    def mate_send(o, s):
        start(lambda: remote(xall.at[o, 0, strip(s)], xall.at[o, 1, strip(s)],
                             md_send.at[o, s], md_recv.at[o, s], partner))

    def ring_arrived(o, s):
        remote(xall.at[o, 0, strip(s)], xall.at[o, 0, strip(s)],
               ag_send.at[o, s], ag_recv.at[o, s], right).wait_recv()
        mate_send(o, s)

    def mate_arrived(o, p):
        for s in (2 * p, 2 * p + 1):
            remote(xall.at[o, 1, strip(s)], xall.at[o, 1, strip(s)],
                   md_send.at[o, s], md_recv.at[o, s], partner).wait_recv()

    for i in (0, 1):
        x_copies[2 * i].wait()
        ring_send(0, 3, i, right)
        x_copies[2 * i + 1].wait()
        ring_send(0, 1, i + 4, left)
    for copy in x_copies[4:]:
        copy.wait()
    for i in range(STRIPS):
        mate_send(0, i)
    for copy in w_copies:
        copy.start()
    for copy in in_copies:
        copy.wait()
    build_table(ids, gates, hot_ref, hot_g_ref, tab_ref, experts)
    for device, o, q in peers:
        start(functools.partial(remote, tab_ref.at[device, pl.ds(0, experts)],
                                tabs.at[(CHIPS - o) % CHIPS, q, pl.ds(0, experts)], tb_send.at[o, q],
                                tb_recv.at[(CHIPS - o) % CHIPS, q], device))
    tabs[0, 0] = tab_ref[me]

    lane = lax.broadcasted_iota(jnp.int32, (rows, LANES), 1)

    def gates_ready(o, q):
        if o or q:
            remote(tabs.at[o, q, pl.ds(0, experts)], tabs.at[o, q, pl.ds(0, experts)], tb_send.at[o, q], tb_recv.at[o, q], partner).wait_recv()
        gcol[o, q] = jnp.transpose(tabs[o, q])

    def run_chunk(pairs, first, last, hooks, unroll=False):
        groups = [(o, q, p) for o, p in pairs for q in range(2)]
        if first == 0:
            for o, q, p in groups:
                part[o, q, piece(p)] = jnp.zeros((rows, part.shape[3]), jnp.float32)

        def call_hooks(at):
            for step, hook in hooks:
                if not unroll:
                    pl.when(at == step)(hook)
                elif at == step:
                    hook()

        def body(e, _):
            call_hooks(e)
            if (pairs, first) == ([(0, 0), (0, 2)], 0):
                for i in range(3):
                    ref = (wg, wu, wd)[i]
                    pltpu.make_async_copy(ref.at[e], ref.at[e], w_sem.at[3 * e + i]).wait()
            x = jnp.concatenate([xall[o, q, piece(p)] for o, q, p in groups], axis=0)
            half = wg.shape[2] // 2
            hidden = []
            for n in range(2):
                cols = pl.ds(n * half, half)
                a = jnp.dot(x, wg[e, :, cols], preferred_element_type=jnp.float32)
                b = jnp.dot(x, wu[e, :, cols], preferred_element_type=jnp.float32)
                hidden.append((a * jax.nn.sigmoid(a) * b).astype(jnp.bfloat16))
            if unroll:
                call_hooks(e + 0.5)
            u = jnp.concatenate(hidden, axis=1)
            weight = [jnp.sum(jnp.where(lane == e, gcol[o, q, piece(p)], 0.0), axis=1, keepdims=True)
                      for o, q, p in groups]
            width = 512
            for n in range(wd.shape[2] // width):
                cols = pl.ds(n * width, width)
                h = jnp.dot(u, wd[e, :, cols], preferred_element_type=jnp.float32).astype(jnp.bfloat16).astype(jnp.float32)
                for i, (o, q, p) in enumerate(groups):
                    hi = h[i * rows:(i + 1) * rows]
                    part[o, q, piece(p), cols] += jnp.where(weight[i] != 0, weight[i] * hi, 0.0)
            return 0

        if unroll:
            for e in range(first, last):
                body(e, 0)
        else:
            lax.fori_loop(first, last, body, 0)
        for o, p in pairs if last == experts else ():
            start(functools.partial(remote, part.at[o, 1, piece(p)], mate.at[o, piece(p)],
                                    pd_send.at[o, p], pd_recv.at[o, p], partner))

    def partner_sum(o, p):
        remote(mate.at[o, piece(p)], mate.at[o, piece(p)], pd_send.at[o, p], pd_recv.at[o, p], partner).wait_recv()
        return part[o, 0, piece(p)] + mate[o, piece(p)]

    def rs_transfer(o, p, device):
        dst = {2: ring, 3: from_right, 1: from_left}[o]
        return remote(part.at[o, 0, piece(p)], dst.at[piece(p)], rs_send.at[o, p], rs_recv.at[o, p], device)

    def finish(o, p):
        total = partner_sum(o, p)
        goes_left = o == 3 or (o == 2 and p < 2)
        if (o == 3 and p < 2) or (o == 1 and p >= 2):
            rs_transfer(2, p, left).wait_recv()
            total = total + ring[piece(p)]
        part[o, 0, piece(p)] = total
        make = functools.partial(rs_transfer, o, p, left if goes_left else right)
        make().start()
        sums_sent.append(make)

    def stage(i):
        def act():
            ring_arrived(3, i)
            ring_send(3, 2, i, right)
            ring_arrived(1, i + 4)
            ring_send(1, 2, i + 4, left)
            for own in ((2,), (3,), (4,), (5, 6, 7))[i]:
                ring_send(0, 3, own, right)
                ring_send(0, 1, (own + 4) % STRIPS, left)
        return act

    def far(i):
        def act():
            for s in (2 * i, 2 * i + 1, 2 * i + 4, 2 * i + 5):
                ring_arrived(2, s)
        return act

    def near(i):
        def act():
            for s in (2 * i, 2 * i + 1):
                ring_arrived(3, s + 4)
                ring_arrived(1, s)
        return act

    def both(o1, p1, o2, p2):
        def act():
            finish(o1, p1)
            finish(o2, p2)
        return act

    def mates(*items):
        for o, p in items:
            mate_arrived(o, p)

    gates_ready(0, 0)
    gates_ready(0, 1)
    mates(*[(0, p) for p in range(QUARTERS)])
    run_chunk([(0, 0), (0, 2)], 0, experts, [(1, stage(0)), (3, stage(1))])
    run_chunk([(0, 1), (0, 3)], 0, 2, [(1, stage(2))])
    far(0)()
    for q in range(2):
        gates_ready(2, q)
    mates((2, 0), (2, 2))
    run_chunk([(2, 0), (2, 2)], 0, experts, [(1, stage(3)), (4, far(1))], True)
    mates((2, 1), (2, 3))
    run_chunk([(2, 1), (2, 3)], 0, experts, [(1.5, both(2, 0, 2, 2)), (3, near(0))], True)
    for o in (1, 3):
        for q in range(2):
            gates_ready(o, q)
    mates((3, 2), (1, 0))
    run_chunk([(3, 2), (1, 0)], 0, experts, [(1.5, both(2, 1, 2, 3)), (2, near(1))], True)
    mates((3, 3), (1, 1))
    run_chunk([(3, 3), (1, 1)], 0, experts, [(1.5, both(3, 2, 1, 0))], True)
    mates((3, 0), (1, 2))
    run_chunk([(3, 0), (1, 2)], 0, experts, [(1.5, both(3, 3, 1, 1))], True)
    mates((3, 1), (1, 3))
    run_chunk([(3, 1), (1, 3)], 0, experts, [(1, both(3, 0, 1, 2))])
    run_chunk([(0, 1), (0, 3)], 2, experts, [(4, both(3, 1, 1, 3))])

    for p in range(QUARTERS):
        part[0, 0, piece(p)] = partner_sum(0, p)
    out_copies = []
    for make in sends + sums_sent[:8]:
        make().wait_send()
    for p in (0, 2, 1, 3):
        rs_transfer(3, p, left).wait_recv()
        rs_transfer(1, p, left).wait_recv()
        total = part[0, 0, piece(p)] + from_right[piece(p)] + from_left[piece(p)]
        out_hbm[piece(p)] = total.astype(out_hbm.dtype)
    for make in sums_sent[8:]:
        make().wait_send()


def solution(mesh):
    group_size = mesh.shape['ep']
    row_spec = P(('dp', 'ep'), None)
    list_spec = P(('dp', 'ep'))
    expert_spec = P('ep', None, None)

    def local_layer(x_loc, ids_loc, gates_loc, hot_loc, hot_g_loc, wg_loc, wu_loc, wd_loc):
        experts, d_model, d_ff = wg_loc.shape
        tokens = x_loc.shape[0]
        top_k = ids_loc.shape[1]
        hot_rows = hot_loc.shape[0]
        any_spec = pl.BlockSpec(memory_space=pl.ANY)
        dma = pltpu.SemaphoreType.DMA
        f32, bf16 = jnp.float32, jnp.bfloat16
        return pl.pallas_call(
            moe_kernel,
            out_shape=pltpu.VMEM(x_loc.shape, x_loc.dtype),
            in_specs=[any_spec] * 8,
            out_specs=pl.BlockSpec(memory_space=pltpu.VMEM),
            scratch_shapes=[
                pltpu.SMEM((hot_rows,), jnp.int32),
                pltpu.SMEM((hot_rows,), f32),
                pltpu.VMEM((top_k, tokens), jnp.int32),
                pltpu.VMEM((top_k, tokens), f32),
                pltpu.VMEM((group_size, LANES, tokens), f32),
                pltpu.VMEM((CHIPS, 2, tokens, d_model), bf16),
                pltpu.VMEM((experts, d_model, d_ff), bf16),
                pltpu.VMEM((experts, d_model, d_ff), bf16),
                pltpu.VMEM((experts, d_ff, d_model), bf16),
                pltpu.VMEM((CHIPS, 2, tokens, d_model), f32),
                pltpu.VMEM((CHIPS, tokens, d_model), f32),
                pltpu.VMEM((tokens, d_model), f32),
                pltpu.VMEM((tokens, d_model), f32),
                pltpu.VMEM((tokens, d_model), f32),
                pltpu.VMEM((CHIPS, 2, LANES, tokens), f32),
                pltpu.VMEM((CHIPS, 2, tokens, LANES), f32),
                dma((3 * experts,)), dma((STRIPS,)), dma((4,)),
                dma((CHIPS, STRIPS)), dma((CHIPS, STRIPS)),
                dma((CHIPS, STRIPS)), dma((CHIPS, STRIPS)),
                dma((CHIPS, 2)), dma((CHIPS, 2)),
                dma((CHIPS, QUARTERS)), dma((CHIPS, QUARTERS)),
                dma((CHIPS, QUARTERS)), dma((CHIPS, QUARTERS)),
            ],
            compiler_params=pltpu.CompilerParams(collective_id=0, has_side_effects=True, vmem_limit_bytes=62_000_000),
            cost_estimate=pl.CostEstimate(flops=100_000_000, bytes_accessed=30_000_000, transcendentals=0),
            name='moe_ring',
        )(hot_loc, hot_g_loc, x_loc, ids_loc.T, gates_loc.T, wg_loc, wu_loc, wd_loc)

    return jax.shard_map(local_layer, mesh=mesh,
                         in_specs=(row_spec, row_spec, row_spec, list_spec, list_spec, expert_spec, expert_spec, expert_spec),
                         out_specs=row_spec, check_vma=False)
```
